32 devices in a mesh: groups: 2 (over y), gx: 4 (over z), gy: 4 (over x, core).
Axes of the slice: x: 2, y: 2, z: 4, core: 2. Of those that a mesh axis runs over, the one named last changes fastest.
Arguments:
- thermal_deviation: float32 [32, 256, 512], P('groups', 'gy', 'gx'), parts along dimension 0, may hold values from -6 to 6
- brine_content: float32 [32, 256, 512], P('groups', 'gy', 'gx'), parts along dimension 0, may hold values from 0.2 to 2.4
- current_components: float32 [4, 16, 256, 512], P('groups', None, 'gy', 'gx'), parts along dimension 0, may hold values from -4 to 4
- sea_indicator: int32 [256, 512], P('gy', 'gx'), may hold values from 0 to 1, as said below
- flooded_layer_number: int32 [256, 512], P('gy', 'gx'), may hold values from 1 to 16
- footprint_square_metres: float32 [256, 512], P('gy', 'gx'), may hold values from 0.5 to 5
- rainfall_input: float32 [256, 512], P('gy', 'gx'), may hold values from -2 to 3.5
- seam_partner_index: int32 [512], P('gx'), may hold values from 0 to 511, as said below
Outputs:
- temperature_next: float32 [32, 256, 512], P('groups', 'gy', 'gx'), parts along dimension 0
- salinity_next: float32 [32, 256, 512], P('groups', 'gy', 'gx'), parts along dimension 0
The draws below stay inside these ranges and needn't reach their ends.
There are 2 independent parts, one for each index of `groups`. The reference program is written for one: setup_inputs(seed, part) draws one part's arguments, and reference() takes and returns one part's arrays. A program takes and returns all parts, laid end to end along the dimension named above; an argument that names none is the same for every part. Nothing has to cross between parts.
Inputs may be any that keep to these rules, and one draw needn't show every extreme that they name: `sea_indicator`: at least one column is ocean. seam_partner_index[x] = (s - x) mod 512 for one s of each draw with s mod 128 = 127; the map is its own inverse and has no fixed point.
All inputs are finite; a program needn't handle non-finite values.
Results may differ from the reference program's by a relative error of at most 0.00002.
Values sent between devices are 32-bit elements; how exact they have to be, the bound alone decides.
A program may use at most 64 MiB of HBM per device.

```python
import math
import jax
import jax.numpy as jnp

SEA_LAYER_TOTAL = 16
CX = 128
PARALLEL_TOTAL = 256
MERIDIAN_TOTAL = 512


def draw_brine_content(key, part):
    longitude = jnp.arange(MERIDIAN_TOTAL, dtype=jnp.float32) / MERIDIAN_TOTAL
    zonal_trend = 0.5 + longitude
    factor = jax.random.uniform(key, (SEA_LAYER_TOTAL, PARALLEL_TOTAL, MERIDIAN_TOTAL), jnp.float32, 0.6, 1.4)
    return (zonal_trend * factor).astype(jnp.float32)


def draw_rainfall_input(key, part):
    second = jax.random.fold_in(jax.random.fold_in(key, 11), 1)
    longitude = jnp.arange(MERIDIAN_TOTAL, dtype=jnp.float32) / MERIDIAN_TOTAL
    zonal_trend = 0.5 + longitude
    rough_noise = jnp.clip(0.5 * jax.random.normal(second, (PARALLEL_TOTAL, MERIDIAN_TOTAL), jnp.float32), -2.0, 2.0)
    return (zonal_trend + rough_noise).astype(jnp.float32)


def draw_sea_indicator(key, part):
    first, second = jax.random.split(jax.random.fold_in(key, 23))
    ocean_draw = (jax.random.randint(first, (PARALLEL_TOTAL, MERIDIAN_TOTAL), 0, 4) < 3).astype(jnp.int32)
    chosen = jax.random.randint(second, (), 0, PARALLEL_TOTAL * MERIDIAN_TOTAL)
    flat_index = jnp.arange(PARALLEL_TOTAL * MERIDIAN_TOTAL, dtype=jnp.int32).reshape(PARALLEL_TOTAL, MERIDIAN_TOTAL)
    return jnp.where(flat_index == chosen, 1, ocean_draw).astype(jnp.int32)


def draw_seam_partner_index(key, part):
    block_choice = jax.random.randint(jax.random.fold_in(key, 37), (), 0, MERIDIAN_TOTAL // CX)
    centre = CX * block_choice + CX - 1
    return ((centre - jnp.arange(MERIDIAN_TOTAL, dtype=jnp.int32)) % MERIDIAN_TOTAL).astype(jnp.int32)


def place_ends(drawn, stream_key, low, top_value):
    place = [jax.random.randint(jax.random.fold_in(stream_key, axis), (), 0, length) for axis, length in enumerate(drawn.shape)]
    widest = drawn.shape.index(max(drawn.shape))
    beside = place[:widest] + [(place[widest] + 1) % drawn.shape[widest]] + place[widest + 1:]
    return drawn.at[tuple(place)].set(low).at[tuple(beside)].set(top_value)


def shard_levels(stream_key, shape, cuts, least, largest):
    level, own = 1.0, jax.random.fold_in(stream_key, 6)
    for position, blocks in cuts:
        draws = jnp.exp(jax.random.uniform(jax.random.fold_in(own, position), (blocks,), jnp.float32, least / len(cuts), largest / len(cuts)))
        level = level * jnp.repeat(draws, shape[position] // blocks).reshape([-1 if axis == position else 1 for axis in range(len(shape))])
    return level


def noise(rng, dims, scale, bound, pieces=(), kind=jnp.bfloat16):
    entries = scale * jax.random.normal(rng, dims, jnp.float32)
    if pieces:
        entries = entries * shard_levels(rng, dims, pieces, -0.22, 0.18)
    return jnp.clip(entries, -bound, bound).astype(kind)


def setup_inputs(seed: int = 0, part: int = 0) -> dict:
    splits = jax.random.split(jax.random.key(seed), 9)
    part_keys = jax.random.split(jax.random.fold_in(splits[8], part), 9)
    thermal_deviation = noise(part_keys[0], (SEA_LAYER_TOTAL, PARALLEL_TOTAL, MERIDIAN_TOTAL), 1.0, 6.0, ((1, 4), (2, 4)), jnp.float32)
    brine_content = draw_brine_content(jax.random.fold_in(jax.random.fold_in(splits[8], part), 71), part)
    current_components = noise(part_keys[2], (2, SEA_LAYER_TOTAL, PARALLEL_TOTAL, MERIDIAN_TOTAL), 1.0, 4.0, ((2, 4), (3, 4)), jnp.float32)
    sea_indicator = draw_sea_indicator(jax.random.fold_in(splits[8], 71), part)
    flooded_layer_number = place_ends(jax.random.randint(splits[4], (PARALLEL_TOTAL, MERIDIAN_TOTAL), 1, SEA_LAYER_TOTAL + 1), jax.random.fold_in(splits[4], 1), 1, SEA_LAYER_TOTAL).astype(jnp.int32)
    footprint_square_metres = jnp.clip(jnp.exp(math.log(5.0) - 2.3025851 * jax.random.uniform(splits[5], (PARALLEL_TOTAL, MERIDIAN_TOTAL), jnp.float32) ** shard_levels(splits[5], (PARALLEL_TOTAL, MERIDIAN_TOTAL), ((0, 4), (1, 4)), -0.2, 0.2)), 0.5, 5.0)
    rainfall_input = draw_rainfall_input(jax.random.fold_in(splits[8], 71), part)
    seam_partner_index = draw_seam_partner_index(jax.random.fold_in(splits[8], 71), part)
    return {"thermal_deviation": thermal_deviation, "brine_content": brine_content, "current_components": current_components, "sea_indicator": sea_indicator, "flooded_layer_number": flooded_layer_number, "footprint_square_metres": footprint_square_metres, "rainfall_input": rainfall_input, "seam_partner_index": seam_partner_index}


time_step = 0.25
diffusivity = 0.5
vertical_mixing = 0.3
top_thickness = 0.5


def face_flux(near_cells, far_cells, face_speed, near_wet, far_wet):
    upwind = jnp.maximum(face_speed, 0.0) * near_cells + jnp.minimum(face_speed, 0.0) * far_cells
    return near_wet * far_wet * (upwind - diffusivity * (far_cells - near_cells))


def reference(thermal_deviation, brine_content, current_components, sea_indicator, flooded_layer_number, footprint_square_metres, rainfall_input, seam_partner_index):
    layer_stack_number = thermal_deviation.shape[0]
    stacked_layer_number = (sea_indicator * flooded_layer_number).astype(jnp.float32)
    level_index = jnp.arange(layer_stack_number, dtype=jnp.float32)
    wet_cells = (level_index[:, None, None] < stacked_layer_number[None]).astype(jnp.float32)
    carried_quantity = jnp.stack([thermal_deviation, brine_content])
    east_tracer = jnp.roll(carried_quantity, -1, axis=3)
    east_wet = jnp.roll(wet_cells, -1, axis=2)
    east_flux = face_flux(carried_quantity, east_tracer, current_components[0], wet_cells, east_wet)
    west_flux = jnp.roll(east_flux, 1, axis=3)
    fold_tracer = carried_quantity[:, :, -1, :][:, :, seam_partner_index]
    fold_wet = wet_cells[:, -1, :][:, seam_partner_index]
    fold_velocity = current_components[1][:, -1, :][:, seam_partner_index]
    north_tracer = jnp.concatenate([carried_quantity[:, :, 1:], fold_tracer[:, :, None]], axis=2)
    north_wet = jnp.concatenate([wet_cells[:, 1:], fold_wet[:, None]], axis=1)
    fold_speed = 0.5 * (current_components[1][:, -1, :] - fold_velocity)
    north_speed = jnp.concatenate([current_components[1][:, :-1], fold_speed[:, None]], axis=1)
    north_flux = face_flux(carried_quantity, north_tracer, north_speed, wet_cells, north_wet)
    south_flux = jnp.concatenate([jnp.zeros_like(north_flux[:, :, :1]), north_flux[:, :, :-1]], axis=2)
    vertical = wet_cells[:-1] * wet_cells[1:] * vertical_mixing * (carried_quantity[:, :-1] - carried_quantity[:, 1:])
    zero_layer = jnp.zeros_like(vertical[:, :1])
    from_above = jnp.concatenate([zero_layer, vertical], axis=1)
    to_below = jnp.concatenate([vertical, zero_layer], axis=1)
    tendency = time_step / footprint_square_metres * (west_flux - east_flux + south_flux - north_flux) + time_step * (from_above - to_below)
    updated = carried_quantity + wet_cells * tendency
    wet_area = footprint_square_metres * sea_indicator.astype(jnp.float32)
    total_area = jnp.sum(wet_area)
    mean_fresh = jnp.sum(wet_area * rainfall_input) / total_area
    balanced = rainfall_input - mean_fresh
    surface = brine_content[0]
    total_salt = jnp.sum(wet_area * surface * balanced)
    virtual = -surface * balanced + total_salt / total_area
    surface_next = updated[1, 0] + time_step / top_thickness * virtual * wet_cells[0]
    salinity_next = jnp.concatenate([surface_next[None], updated[1, 1:]], axis=0)
    return (updated[0], salinity_next)
```

```python
import functools

import jax
import jax.numpy as jnp
from jax import lax
from jax.experimental import pallas as pl
from jax.experimental.pallas import tpu as pltpu
from jax.sharding import PartitionSpec as P

time_step = 0.25
diffusivity = 0.5
vertical_mixing = 0.3
top_thickness = 0.5

MESH = pl.DeviceIdType.MESH


def repeat(count, body):
    if count <= 16:
        for i in range(count):
            body(i)
    else:
        pl.loop(0, count)(body)


def face_weights(speed, open_face):
    near_weight = jnp.where(open_face, jnp.maximum(speed, 0.0) + diffusivity, 0.0)
    far_weight = jnp.where(open_face, jnp.minimum(speed, 0.0) - diffusivity, 0.0)
    return near_weight, far_weight


def kernel(
    nx, ny, nk, h, w,
    t_hbm, s_hbm, uv_hbm, sea_hbm, lay_hbm, area_hbm, rain_hbm, seam_smem,
    t_out, s_out,
    t_v, s_v, uv_v, sea_v, lay_v, area_v, rain_v, s0_v, g_v, depth_v,
    pack_v, east_v, west_v, up_v, down_v, south_v, north_v, fold_v, part_v, parts_v,
    load_sems, pack_send, pack_recv, row_send, row_recv, fold_send, fold_recv,
    part_send, part_recv,
):
    mx, my = lax.axis_index("gx"), lax.axis_index("gy")
    is_top = my == ny - 1
    peers = nx * ny - 1

    def peer(r):
        r = r + 1
        return {"gx": lax.rem(mx + r // ny, nx), "gy": lax.rem(my + r % ny, ny)}

    barrier = pltpu.get_barrier_semaphore()

    def greet(r):
        pl.semaphore_signal(barrier, inc=1, device_id=peer(r), device_id_type=MESH)

    repeat(peers, greet)

    loads = [
        pltpu.make_async_copy(src, dst, load_sems.at[i])
        for i, (src, dst) in enumerate(
            [
                (area_hbm, area_v),
                (sea_hbm, sea_v),
                (rain_hbm, rain_v),
                (s_hbm.at[pl.ds(0, h)], s0_v),
                (lay_hbm, lay_v),
                (t_hbm, t_v),
                (s_hbm, s_v),
                (uv_hbm.at[pl.ds(0, nk * h)], uv_v.at[pl.ds(0, nk * h)]),
                (uv_hbm.at[pl.ds(nk * h, nk * h)], uv_v.at[pl.ds(nk * h, nk * h)]),
            ]
        )
    ]
    for load in loads:
        load.start()

    for load in loads[:4]:
        load.wait()
    area = area_v[...]
    sea = sea_v[...]
    wet_area = area * sea.astype(jnp.float32)
    surface = s0_v[...]
    fresh = wet_area * rain_v[...]
    row8 = lax.broadcasted_iota(jnp.int32, (8, w), 0)
    part = jnp.zeros((8, w), jnp.float32)
    for i, term in enumerate((wet_area, fresh, fresh * surface, wet_area * surface)):
        part = jnp.where(row8 == i, jnp.sum(term, axis=0, keepdims=True), part)
    part_v[...] = part
    gain = time_step / area
    g_v[...] = gain

    for load in loads[4:]:
        load.wait()
    depth = (sea * lay_v[...]).astype(jnp.float32)
    depth_v[...] = depth

    lane = lax.broadcasted_iota(jnp.int32, (h, w), 1)
    pair = lane // 2
    packed = jnp.zeros((h, w), jnp.float32)
    for i, ref in enumerate((t_v, s_v, uv_v)):
        for k in range(nk):
            j = i * nk + k
            packed = jnp.where(pair == j, pltpu.roll(ref[pl.ds(k * h, h), :], 2 * j + 1, 1), packed)
    depth_at = 6 * nk
    packed = jnp.where(pair == 3 * nk, pltpu.roll(depth, depth_at + 1, 1), packed)
    pack_v[...] = packed

    def rows(ref, row, base=0):
        return ref[pl.ds(base + row, nk, stride=h), :]

    up_v[pl.ds(0, nk), :] = rows(t_v, h - 1)
    up_v[pl.ds(nk, nk), :] = rows(s_v, h - 1)
    up_v[pl.ds(2 * nk, nk), :] = rows(uv_v, h - 1, nk * h)
    up_v[pl.ds(3 * nk, 8), :] = jnp.broadcast_to(depth[h - 1 : h, :], (8, w))
    down_v[pl.ds(0, nk), :] = rows(t_v, 0)
    down_v[pl.ds(nk, nk), :] = rows(s_v, 0)
    down_v[pl.ds(2 * nk, 8), :] = jnp.broadcast_to(depth[0:1, :], (8, w))

    @pl.when(is_top)
    def _():
        up = up_v[...]
        flip = (w - 1) - lax.broadcasted_iota(jnp.int32, up.shape, 1)
        fold_v[mx] = jnp.take_along_axis(up, flip, axis=1)

    pl.semaphore_wait(barrier, peers)

    def part_copy(r):
        return pltpu.make_async_remote_copy(
            src_ref=part_v, dst_ref=parts_v.at[r],
            send_sem=part_send.at[r], recv_sem=part_recv.at[r],
            device_id=peer(r), device_id_type=MESH,
        )

    repeat(peers, lambda r: part_copy(r).start())

    to_east = pltpu.make_async_remote_copy(
        src_ref=pack_v, dst_ref=west_v, send_sem=pack_send.at[0], recv_sem=pack_recv.at[0],
        device_id={"gx": lax.rem(mx + 1, nx)}, device_id_type=MESH,
    )
    to_west = pltpu.make_async_remote_copy(
        src_ref=pack_v, dst_ref=east_v, send_sem=pack_send.at[1], recv_sem=pack_recv.at[1],
        device_id={"gx": lax.rem(mx + nx - 1, nx)}, device_id_type=MESH,
    )
    to_north = pltpu.make_async_remote_copy(
        src_ref=up_v, dst_ref=south_v, send_sem=row_send.at[0], recv_sem=row_recv.at[0],
        device_id={"gy": lax.rem(my + 1, ny)}, device_id_type=MESH,
    )
    to_south = pltpu.make_async_remote_copy(
        src_ref=down_v, dst_ref=north_v, send_sem=row_send.at[1], recv_sem=row_recv.at[1],
        device_id={"gy": lax.rem(my + ny - 1, ny)}, device_id_type=MESH,
    )

    def fold_copy(d):
        return pltpu.make_async_remote_copy(
            src_ref=fold_v.at[mx], dst_ref=fold_v.at[mx],
            send_sem=fold_send.at[d], recv_sem=fold_recv.at[d],
            device_id={"gx": lax.rem(mx + d + 1, nx)}, device_id_type=MESH,
        )

    to_east.start()
    to_west.start()

    @pl.when(jnp.logical_not(is_top))
    def _():
        to_north.start()

    @pl.when(my > 0)
    def _():
        to_south.start()

    @pl.when(is_top)
    def _():
        repeat(nx - 1, lambda d: fold_copy(d).start())

    row = lax.broadcasted_iota(jnp.int32, (h, w), 0)
    depth_east = jnp.where(lane == w - 1, 0.0, jnp.minimum(depth, pltpu.roll(depth, w - 1, 1)))
    depth_north = jnp.where(row == h - 1, 0.0, jnp.minimum(depth, pltpu.roll(depth, h - 1, 0)))

    def level(k, above):
        kf = k.astype(jnp.float32)
        at = pl.ds(pl.multiple_of(k * h, h), h)
        below = pl.ds(pl.multiple_of(jnp.minimum(k + 1, nk - 1) * h, h), h)
        east_near, east_far = face_weights(uv_v[at, :], depth_east > kf)
        north_near, north_far = face_weights(
            uv_v[pl.ds(pl.multiple_of((k + nk) * h, h), h), :], depth_north > kf
        )
        mix = jnp.where(depth_v[...] > kf + 1.0, time_step * vertical_mixing, 0.0)
        gain = g_v[...]
        falls = []
        for ref, out, came in ((t_v, t_out, above[0]), (s_v, s_out, above[1])):
            c = ref[at, :]
            east = east_near * c + east_far * pltpu.roll(c, w - 1, 1)
            north = north_near * c + north_far * pltpu.roll(c, h - 1, 0)
            flow = (pltpu.roll(east, 1, 1) - east) + (pltpu.roll(north, 1, 0) - north)
            fall = mix * (c - ref[below, :])
            out[at, :] = c + (gain * flow + (came - fall))
            falls.append(fall)
        return tuple(falls)

    zero = jnp.zeros((h, w), jnp.float32)
    lax.fori_loop(0, nk, level, (zero, zero))

    to_east.wait()
    to_west.wait()
    mine, east_side, west_side = pack_v[...], east_v[...], west_v[...]
    even = lane % 2 == 0

    def speeds(cells):
        return jnp.where(
            pair < nk, pltpu.roll(cells, w - 4 * nk, 1), pltpu.roll(cells, w - 2 * nk, 1)
        )

    def column(cells, at):
        return jnp.broadcast_to(cells[:, at : at + 1], (h, w))

    near = jnp.where(even, mine, pltpu.roll(west_side, 1, 1))
    far = jnp.where(even, pltpu.roll(east_side, w - 1, 1), mine)
    speed = jnp.where(even, speeds(mine), pltpu.roll(speeds(west_side), 1, 1))
    shallow = jnp.where(
        even,
        jnp.minimum(column(mine, depth_at), column(east_side, depth_at + 1)),
        jnp.minimum(column(mine, depth_at + 1), column(west_side, depth_at)),
    )
    near_weight, far_weight = face_weights(speed, shallow > (pair % nk).astype(jnp.float32))
    gain = g_v[...]
    edge_gain = jnp.where(even, -column(gain, w - 1), column(gain, 0))
    edge = edge_gain * (near_weight * near + far_weight * far)
    at_edge = (lane == 0) | (lane == w - 1)
    for i, out in enumerate((t_out, s_out)):
        for k in range(nk):
            shift = (w - (2 * (i * nk + k) + 1)) % w
            out[pl.ds(k * h, h), :] += jnp.where(at_edge, pltpu.roll(edge, shift, 1), 0.0)

    level_row = lax.broadcasted_iota(jnp.int32, (nk, w), 0).astype(jnp.float32)

    def north_edge(far_t, far_s, speed, far_depth):
        near_weight, far_weight = face_weights(
            speed, jnp.minimum(up_v[3 * nk : 3 * nk + 1, :], far_depth) > level_row
        )
        for near, far, out in (
            (up_v[pl.ds(0, nk), :], far_t, t_out),
            (up_v[pl.ds(nk, nk), :], far_s, s_out),
        ):
            at = pl.ds(h - 1, nk, stride=h)
            out[at, :] -= g_v[h - 1 : h, :] * (near_weight * near + far_weight * far)

    @pl.when(is_top)
    def _():
        repeat(nx - 1, lambda d: fold_copy(d).wait())
        partner = fold_v[seam_smem[0] // w]
        north_edge(
            partner[:nk],
            partner[nk : 2 * nk],
            0.5 * (up_v[pl.ds(2 * nk, nk), :] - partner[2 * nk : 3 * nk]),
            partner[3 * nk : 3 * nk + 1],
        )

    @pl.when(jnp.logical_not(is_top))
    def _():
        to_north.wait_send()
        to_south.wait_recv()
        north_edge(
            north_v[pl.ds(0, nk), :],
            north_v[pl.ds(nk, nk), :],
            up_v[pl.ds(2 * nk, nk), :],
            north_v[2 * nk : 2 * nk + 1, :],
        )

    @pl.when(my > 0)
    def _():
        to_south.wait_send()
        to_north.wait_recv()
        near_weight, far_weight = face_weights(
            south_v[pl.ds(2 * nk, nk), :],
            jnp.minimum(down_v[2 * nk : 2 * nk + 1, :], south_v[3 * nk : 3 * nk + 1, :]) > level_row,
        )
        for i, out in enumerate((t_out, s_out)):
            at = pl.ds(0, nk, stride=h)
            out[at, :] += g_v[0:1, :] * (
                near_weight * south_v[pl.ds(i * nk, nk), :]
                + far_weight * down_v[pl.ds(i * nk, nk), :]
            )

    repeat(peers, lambda r: part_copy(r).wait())
    totals = part_v[...] + jnp.sum(parts_v[...], axis=0)
    totals = jnp.sum(totals, axis=1, keepdims=True)
    total_area, total_fresh = totals[0:1], totals[1:2]
    salt_fresh, salt_only = totals[2:3], totals[3:4]
    mean_fresh = total_fresh / total_area
    lift = (salt_fresh - mean_fresh * salt_only) / total_area
    virtual = lift - s0_v[...] * (rain_v[...] - mean_fresh)
    s_out[pl.ds(0, h), :] += jnp.where(depth_v[...] > 0.0, time_step / top_thickness * virtual, 0.0)


def shards(nx, ny, t, s, uv, sea, layers, area, rain, seam):
    nk, h, w = t.shape
    assert w == 128 and h % 8 == 0 and nk % 8 == 0 and 6 * nk + 2 <= w
    f32 = jnp.float32
    peers = nx * ny - 1
    any_space = pl.BlockSpec(memory_space=pl.ANY)
    dma = pltpu.SemaphoreType.DMA
    plane = pltpu.VMEM((h, w), f32)
    t_next, s_next = pl.pallas_call(
        functools.partial(kernel, nx, ny, nk, h, w),
        out_shape=[jax.ShapeDtypeStruct((nk * h, w), f32)] * 2,
        in_specs=[any_space] * 7 + [pl.BlockSpec(memory_space=pltpu.SMEM)],
        out_specs=[pl.BlockSpec(memory_space=pltpu.VMEM)] * 2,
        scratch_shapes=[
            pltpu.VMEM((nk * h, w), f32),
            pltpu.VMEM((nk * h, w), f32),
            pltpu.VMEM((2 * nk * h, w), f32),
            pltpu.VMEM((h, w), jnp.int32),
            pltpu.VMEM((h, w), jnp.int32),
            plane, plane, plane, plane, plane,
            plane, plane, plane,
            pltpu.VMEM((3 * nk + 8, w), f32),
            pltpu.VMEM((2 * nk + 8, w), f32),
            pltpu.VMEM((3 * nk + 8, w), f32),
            pltpu.VMEM((2 * nk + 8, w), f32),
            pltpu.VMEM((nx, 3 * nk + 8, w), f32),
            pltpu.VMEM((8, w), f32),
            pltpu.VMEM((peers, 8, w), f32),
            dma((9,)), dma((2,)), dma((2,)), dma((2,)), dma((2,)),
            dma((nx - 1,)), dma((nx - 1,)), dma((peers,)), dma((peers,)),
        ],
        compiler_params=pltpu.CompilerParams(collective_id=0, has_side_effects=True),
        name="tracer_step",
    )(
        t.reshape(nk * h, w), s.reshape(nk * h, w), uv.reshape(2 * nk * h, w),
        sea, layers, area, rain, seam,
    )
    return t_next.reshape(t.shape), s_next.reshape(s.shape)


def solution(mesh):
    in_specs = (
        P("groups", "gy", "gx"),
        P("groups", "gy", "gx"),
        P("groups", None, "gy", "gx"),
        P("gy", "gx"),
        P("gy", "gx"),
        P("gy", "gx"),
        P("gy", "gx"),
        P("gx"),
    )
    out_specs = (P("groups", "gy", "gx"), P("groups", "gy", "gx"))
    return jax.shard_map(
        functools.partial(shards, mesh.shape["gx"], mesh.shape["gy"]),
        mesh=mesh, in_specs=in_specs, out_specs=out_specs, check_vma=False,
    )
```

```python
import functools

import jax
import jax.numpy as jnp
from jax import lax
from jax.experimental import pallas as pl
from jax.experimental.pallas import tpu as pltpu
from jax.sharding import PartitionSpec as P

time_step = 0.25
diffusivity = 0.5
vertical_mixing = 0.3
top_thickness = 0.5

MESH = pl.DeviceIdType.MESH


def repeat(count, body):
    if count <= 16:
        for i in range(count):
            body(i)
    else:
        pl.loop(0, count)(body)


def face_weights(speed, open_face):
    near_weight = jnp.where(open_face, jnp.maximum(speed, 0.0) + diffusivity, 0.0)
    far_weight = jnp.where(open_face, jnp.minimum(speed, 0.0) - diffusivity, 0.0)
    return near_weight, far_weight


def kernel(
    nx, ny, nk, h, w,
    t_hbm, s_hbm, uv_hbm, sea_hbm, lay_hbm, area_hbm, rain_hbm, seam_smem,
    t_out, s_out,
    t_v, s_v, uv_v, sea_v, lay_v, area_v, rain_v, s0_v, g_v, depth_v,
    pack_v, east_v, west_v, up_v, down_v, south_v, north_v, fold_v, part_v, parts_v,
    load_sems, pack_send, pack_recv, row_send, row_recv, fold_send, fold_recv,
    part_send, part_recv,
):
    mx, my = lax.axis_index("gx"), lax.axis_index("gy")
    is_top = my == ny - 1
    peers = nx * ny - 1

    def peer(r):
        r = r + 1
        return {"gx": lax.rem(mx + r // ny, nx), "gy": lax.rem(my + r % ny, ny)}

    barrier = pltpu.get_barrier_semaphore()

    def greet(r):
        pl.semaphore_signal(barrier, inc=1, device_id=peer(r), device_id_type=MESH)

    repeat(peers, greet)

    loads = [
        pltpu.make_async_copy(src, dst, load_sems.at[i])
        for i, (src, dst) in enumerate(
            [
                (area_hbm, area_v),
                (sea_hbm, sea_v),
                (rain_hbm, rain_v),
                (s_hbm.at[pl.ds(0, h)], s0_v),
                (lay_hbm, lay_v),
                (t_hbm, t_v),
                (s_hbm, s_v),
                (uv_hbm.at[pl.ds(0, nk * h)], uv_v.at[pl.ds(0, nk * h)]),
                (uv_hbm.at[pl.ds(nk * h, nk * h)], uv_v.at[pl.ds(nk * h, nk * h)]),
            ]
        )
    ]
    for load in loads:
        load.start()

    for load in loads[:4]:
        load.wait()
    area = area_v[...]
    sea = sea_v[...]
    wet_area = area * sea.astype(jnp.float32)
    surface = s0_v[...]
    fresh = wet_area * rain_v[...]
    row8 = lax.broadcasted_iota(jnp.int32, (8, w), 0)
    part = jnp.zeros((8, w), jnp.float32)
    for i, term in enumerate((wet_area, fresh, fresh * surface, wet_area * surface)):
        part = jnp.where(row8 == i, jnp.sum(term, axis=0, keepdims=True), part)
    part_v[...] = part
    gain = time_step / area
    g_v[...] = gain

    for load in loads[4:]:
        load.wait()
    depth = (sea * lay_v[...]).astype(jnp.float32)
    depth_v[...] = depth

    lane = lax.broadcasted_iota(jnp.int32, (h, w), 1)
    pair = lane // 2
    packed = jnp.zeros((h, w), jnp.float32)
    for i, ref in enumerate((t_v, s_v, uv_v)):
        for k in range(nk):
            j = i * nk + k
            packed = jnp.where(pair == j, pltpu.roll(ref[pl.ds(k * h, h), :], 2 * j + 1, 1), packed)
    depth_at = 6 * nk
    packed = jnp.where(pair == 3 * nk, pltpu.roll(depth, depth_at + 1, 1), packed)
    pack_v[...] = packed

    def rows(ref, row, base=0):
        return ref[pl.ds(base + row, nk, stride=h), :]

    up_v[pl.ds(0, nk), :] = rows(t_v, h - 1)
    up_v[pl.ds(nk, nk), :] = rows(s_v, h - 1)
    up_v[pl.ds(2 * nk, nk), :] = rows(uv_v, h - 1, nk * h)
    up_v[pl.ds(3 * nk, 8), :] = jnp.broadcast_to(depth[h - 1 : h, :], (8, w))
    down_v[pl.ds(0, nk), :] = rows(t_v, 0)
    down_v[pl.ds(nk, nk), :] = rows(s_v, 0)
    down_v[pl.ds(2 * nk, 8), :] = jnp.broadcast_to(depth[0:1, :], (8, w))

    @pl.when(is_top)
    def _():
        up = up_v[...]
        flip = (w - 1) - lax.broadcasted_iota(jnp.int32, up.shape, 1)
        fold_v[mx] = jnp.take_along_axis(up, flip, axis=1)

    pl.semaphore_wait(barrier, peers)

    def part_copy(r):
        return pltpu.make_async_remote_copy(
            src_ref=part_v, dst_ref=parts_v.at[r],
            send_sem=part_send.at[r], recv_sem=part_recv.at[r],
            device_id=peer(r), device_id_type=MESH,
        )

    repeat(peers, lambda r: part_copy(r).start())

    to_east = pltpu.make_async_remote_copy(
        src_ref=pack_v, dst_ref=west_v, send_sem=pack_send.at[0], recv_sem=pack_recv.at[0],
        device_id={"gx": lax.rem(mx + 1, nx)}, device_id_type=MESH,
    )
    to_west = pltpu.make_async_remote_copy(
        src_ref=pack_v, dst_ref=east_v, send_sem=pack_send.at[1], recv_sem=pack_recv.at[1],
        device_id={"gx": lax.rem(mx + nx - 1, nx)}, device_id_type=MESH,
    )
    to_north = pltpu.make_async_remote_copy(
        src_ref=up_v, dst_ref=south_v, send_sem=row_send.at[0], recv_sem=row_recv.at[0],
        device_id={"gy": lax.rem(my + 1, ny)}, device_id_type=MESH,
    )
    to_south = pltpu.make_async_remote_copy(
        src_ref=down_v, dst_ref=north_v, send_sem=row_send.at[1], recv_sem=row_recv.at[1],
        device_id={"gy": lax.rem(my + ny - 1, ny)}, device_id_type=MESH,
    )

    def fold_copy(d):
        return pltpu.make_async_remote_copy(
            src_ref=fold_v.at[mx], dst_ref=fold_v.at[mx],
            send_sem=fold_send.at[d], recv_sem=fold_recv.at[d],
            device_id={"gx": lax.rem(mx + d + 1, nx)}, device_id_type=MESH,
        )

    to_east.start()
    to_west.start()

    @pl.when(jnp.logical_not(is_top))
    def _():
        to_north.start()

    @pl.when(my > 0)
    def _():
        to_south.start()

    @pl.when(is_top)
    def _():
        repeat(nx - 1, lambda d: fold_copy(d).start())

    row = lax.broadcasted_iota(jnp.int32, (h, w), 0)
    depth_east = jnp.where(lane == w - 1, 0.0, jnp.minimum(depth, pltpu.roll(depth, w - 1, 1)))
    depth_north = jnp.where(row == h - 1, 0.0, jnp.minimum(depth, pltpu.roll(depth, h - 1, 0)))

    def level(k, above):
        kf = k.astype(jnp.float32)
        at = pl.ds(pl.multiple_of(k * h, h), h)
        below = pl.ds(pl.multiple_of(jnp.minimum(k + 1, nk - 1) * h, h), h)
        east_near, east_far = face_weights(uv_v[at, :], depth_east > kf)
        north_near, north_far = face_weights(
            uv_v[pl.ds(pl.multiple_of((k + nk) * h, h), h), :], depth_north > kf
        )
        mix = jnp.where(depth_v[...] > kf + 1.0, time_step * vertical_mixing, 0.0)
        gain = g_v[...]
        falls = []
        for ref, out, came in ((t_v, t_out, above[0]), (s_v, s_out, above[1])):
            c = ref[at, :]
            east = east_near * c + east_far * pltpu.roll(c, w - 1, 1)
            north = north_near * c + north_far * pltpu.roll(c, h - 1, 0)
            flow = (pltpu.roll(east, 1, 1) - east) + (pltpu.roll(north, 1, 0) - north)
            fall = mix * (c - ref[below, :])
            out[at, :] = c + (gain * flow + (came - fall))
            falls.append(fall)
        return tuple(falls)

    zero = jnp.zeros((h, w), jnp.float32)
    lax.fori_loop(0, nk, level, (zero, zero))

    to_east.wait()
    to_west.wait()
    mine, east_side, west_side = pack_v[...], east_v[...], west_v[...]
    even = lane % 2 == 0

    def speeds(cells):
        return jnp.where(
            pair < nk, pltpu.roll(cells, w - 4 * nk, 1), pltpu.roll(cells, w - 2 * nk, 1)
        )

    def column(cells, at):
        return jnp.broadcast_to(cells[:, at : at + 1], (h, w))

    near = jnp.where(even, mine, pltpu.roll(west_side, 1, 1))
    far = jnp.where(even, pltpu.roll(east_side, w - 1, 1), mine)
    speed = jnp.where(even, speeds(mine), pltpu.roll(speeds(west_side), 1, 1))
    shallow = jnp.where(
        even,
        jnp.minimum(column(mine, depth_at), column(east_side, depth_at + 1)),
        jnp.minimum(column(mine, depth_at + 1), column(west_side, depth_at)),
    )
    near_weight, far_weight = face_weights(speed, shallow > (pair % nk).astype(jnp.float32))
    gain = g_v[...]
    edge_gain = jnp.where(even, -column(gain, w - 1), column(gain, 0))
    edge = edge_gain * (near_weight * near + far_weight * far)
    at_edge = (lane == 0) | (lane == w - 1)
    for i, out in enumerate((t_out, s_out)):
        for k in range(nk):
            shift = (w - (2 * (i * nk + k) + 1)) % w
            out[pl.ds(k * h, h), :] += jnp.where(at_edge, pltpu.roll(edge, shift, 1), 0.0)

    level_row = lax.broadcasted_iota(jnp.int32, (nk, w), 0).astype(jnp.float32)

    def north_edge(far_t, far_s, speed, far_depth):
        near_weight, far_weight = face_weights(
            speed, jnp.minimum(up_v[3 * nk : 3 * nk + 1, :], far_depth) > level_row
        )
        for near, far, out in (
            (up_v[pl.ds(0, nk), :], far_t, t_out),
            (up_v[pl.ds(nk, nk), :], far_s, s_out),
        ):
            at = pl.ds(h - 1, nk, stride=h)
            out[at, :] -= g_v[h - 1 : h, :] * (near_weight * near + far_weight * far)

    @pl.when(is_top)
    def _():
        repeat(nx - 1, lambda d: fold_copy(d).wait())
        partner = fold_v[seam_smem[0] // w]
        north_edge(
            partner[:nk],
            partner[nk : 2 * nk],
            0.5 * (up_v[pl.ds(2 * nk, nk), :] - partner[2 * nk : 3 * nk]),
            partner[3 * nk : 3 * nk + 1],
        )

    @pl.when(jnp.logical_not(is_top))
    def _():
        to_north.wait_send()
        to_south.wait_recv()
        north_edge(
            north_v[pl.ds(0, nk), :],
            north_v[pl.ds(nk, nk), :],
            up_v[pl.ds(2 * nk, nk), :],
            north_v[2 * nk : 2 * nk + 1, :],
        )

    @pl.when(my > 0)
    def _():
        to_south.wait_send()
        to_north.wait_recv()
        near_weight, far_weight = face_weights(
            south_v[pl.ds(2 * nk, nk), :],
            jnp.minimum(down_v[2 * nk : 2 * nk + 1, :], south_v[3 * nk : 3 * nk + 1, :]) > level_row,
        )
        for i, out in enumerate((t_out, s_out)):
            at = pl.ds(0, nk, stride=h)
            out[at, :] += g_v[0:1, :] * (
                near_weight * south_v[pl.ds(i * nk, nk), :]
                + far_weight * down_v[pl.ds(i * nk, nk), :]
            )

    repeat(peers, lambda r: part_copy(r).wait())
    totals = part_v[...] + jnp.sum(parts_v[...], axis=0)
    totals = jnp.sum(totals, axis=1, keepdims=True)
    total_area, total_fresh = totals[0:1], totals[1:2]
    salt_fresh, salt_only = totals[2:3], totals[3:4]
    mean_fresh = total_fresh / total_area
    lift = (salt_fresh - mean_fresh * salt_only) / total_area
    virtual = lift - s0_v[...] * (rain_v[...] - mean_fresh)
    s_out[pl.ds(0, h), :] += jnp.where(depth_v[...] > 0.0, time_step / top_thickness * virtual, 0.0)


store_cuts = 4


def store_kernel(t_ref, s_ref, t_out, s_out, sems):
    step = t_ref.shape[0] // store_cuts
    copies = [
        pltpu.make_async_copy(
            src.at[pl.ds(i * step, step)], dst.at[pl.ds(i * step, step)], sems.at[2 * i + n]
        )
        for i in range(store_cuts)
        for n, (src, dst) in enumerate(((t_ref, t_out), (s_ref, s_out)))
    ]
    for copy in copies:
        copy.start()
    for copy in copies:
        copy.wait()


def shards(nx, ny, t, s, uv, sea, layers, area, rain, seam):
    nk, h, w = t.shape
    assert w == 128 and h % 8 == 0 and nk % 8 == 0 and 6 * nk + 2 <= w
    f32 = jnp.float32
    peers = nx * ny - 1
    any_space = pl.BlockSpec(memory_space=pl.ANY)
    dma = pltpu.SemaphoreType.DMA
    plane = pltpu.VMEM((h, w), f32)
    t_next, s_next = pl.pallas_call(
        functools.partial(kernel, nx, ny, nk, h, w),
        out_shape=[pltpu.VMEM((nk * h, w), f32)] * 2,
        in_specs=[any_space] * 7 + [pl.BlockSpec(memory_space=pltpu.SMEM)],
        out_specs=[pl.BlockSpec(memory_space=pltpu.VMEM)] * 2,
        scratch_shapes=[
            pltpu.VMEM((nk * h, w), f32),
            pltpu.VMEM((nk * h, w), f32),
            pltpu.VMEM((2 * nk * h, w), f32),
            pltpu.VMEM((h, w), jnp.int32),
            pltpu.VMEM((h, w), jnp.int32),
            plane, plane, plane, plane, plane,
            plane, plane, plane,
            pltpu.VMEM((3 * nk + 8, w), f32),
            pltpu.VMEM((2 * nk + 8, w), f32),
            pltpu.VMEM((3 * nk + 8, w), f32),
            pltpu.VMEM((2 * nk + 8, w), f32),
            pltpu.VMEM((nx, 3 * nk + 8, w), f32),
            pltpu.VMEM((8, w), f32),
            pltpu.VMEM((peers, 8, w), f32),
            dma((9,)), dma((2,)), dma((2,)), dma((2,)), dma((2,)),
            dma((nx - 1,)), dma((nx - 1,)), dma((peers,)), dma((peers,)),
        ],
        compiler_params=pltpu.CompilerParams(
            collective_id=0, has_side_effects=True, vmem_limit_bytes=65990000
        ),
        name="tracer_step",
    )(
        t.reshape(nk * h, w), s.reshape(nk * h, w), uv.reshape(2 * nk * h, w),
        sea, layers, area, rain, seam,
    )
    t_next, s_next = pl.pallas_call(
        store_kernel,
        out_shape=[jax.ShapeDtypeStruct((nk * h, w), f32)] * 2,
        in_specs=[any_space] * 2,
        out_specs=[any_space] * 2,
        scratch_shapes=[dma((2 * store_cuts,))],
        compiler_params=pltpu.CompilerParams(vmem_limit_bytes=8 << 20),
        name="store",
    )(t_next, s_next)
    return t_next.reshape(t.shape), s_next.reshape(s.shape)


def solution(mesh):
    in_specs = (
        P("groups", "gy", "gx"),
        P("groups", "gy", "gx"),
        P("groups", None, "gy", "gx"),
        P("gy", "gx"),
        P("gy", "gx"),
        P("gy", "gx"),
        P("gy", "gx"),
        P("gx"),
    )
    out_specs = (P("groups", "gy", "gx"), P("groups", "gy", "gx"))
    return jax.shard_map(
        functools.partial(shards, mesh.shape["gx"], mesh.shape["gy"]),
        mesh=mesh, in_specs=in_specs, out_specs=out_specs, check_vma=False,
    )
```

```python
import functools

import jax
import jax.numpy as jnp
from jax import lax
from jax.experimental import pallas as pl
from jax.experimental.pallas import tpu as pltpu
from jax.sharding import PartitionSpec as P

time_step = 0.25
diffusivity = 0.5
vertical_mixing = 0.3
top_thickness = 0.5

MESH = pl.DeviceIdType.MESH


def repeat(count, body):
    if count <= 16:
        for i in range(count):
            body(i)
    else:
        pl.loop(0, count)(body)


def face_weights(speed, open_face):
    near_weight = jnp.where(open_face, jnp.maximum(speed, 0.0) + diffusivity, 0.0)
    far_weight = jnp.where(open_face, jnp.minimum(speed, 0.0) - diffusivity, 0.0)
    return near_weight, far_weight


def kernel(
    nx, ny, nk, h, w,
    t_hbm, s_hbm, uv_hbm, sea_hbm, lay_hbm, area_hbm, rain_hbm, seam_smem,
    t_out, s_out,
    t_v, s_v, uv_v, sea_v, lay_v, area_v, rain_v, s0_v, g_v, depth_v,
    pack_v, last_v, first_v, east_v, west_v, up_v, down_v, south_v, north_v, fold_v,
    part_v, parts_v,
    load_sems, pack_send, pack_recv, row_send, row_recv, fold_send, fold_recv,
    part_send, part_recv,
):
    mx, my = lax.axis_index("gx"), lax.axis_index("gy")
    is_top = my == ny - 1
    peers = nx * ny - 1

    def peer(r):
        r = r + 1
        return {"gx": lax.rem(mx + r // ny, nx), "gy": lax.rem(my + r % ny, ny)}

    barrier = pltpu.get_barrier_semaphore()

    def greet(r):
        pl.semaphore_signal(barrier, inc=1, device_id=peer(r), device_id_type=MESH)

    repeat(peers, greet)

    loads = [
        pltpu.make_async_copy(src, dst, load_sems.at[i])
        for i, (src, dst) in enumerate(
            [
                (area_hbm, area_v),
                (sea_hbm, sea_v),
                (rain_hbm, rain_v),
                (s_hbm.at[pl.ds(0, h)], s0_v),
                (lay_hbm, lay_v),
                (t_hbm, t_v),
                (s_hbm, s_v),
                (uv_hbm.at[pl.ds(0, nk * h)], uv_v.at[pl.ds(0, nk * h)]),
                (uv_hbm.at[pl.ds(nk * h, nk * h)], uv_v.at[pl.ds(nk * h, nk * h)]),
            ]
        )
    ]
    for load in loads:
        load.start()

    for load in loads[:4]:
        load.wait()
    area = area_v[...]
    sea = sea_v[...]
    wet_area = area * sea.astype(jnp.float32)
    surface = s0_v[...]
    fresh = wet_area * rain_v[...]
    row8 = lax.broadcasted_iota(jnp.int32, (8, w), 0)
    part = jnp.zeros((8, w), jnp.float32)
    for i, term in enumerate((wet_area, fresh, fresh * surface, wet_area * surface)):
        part = jnp.where(row8 == i, jnp.sum(term, axis=0, keepdims=True), part)
    part_v[...] = part
    gain = time_step / area
    g_v[...] = gain

    pl.semaphore_wait(barrier, peers)

    def part_copy(r):
        return pltpu.make_async_remote_copy(
            src_ref=part_v, dst_ref=parts_v.at[r],
            send_sem=part_send.at[r], recv_sem=part_recv.at[r],
            device_id=peer(r), device_id_type=MESH,
        )

    repeat(peers, lambda r: part_copy(r).start())

    for load in loads[4:]:
        load.wait()
    depth = (sea * lay_v[...]).astype(jnp.float32)
    depth_v[...] = depth

    lane = lax.broadcasted_iota(jnp.int32, (h, w), 1)
    pair = lane // 2
    packed = jnp.zeros((h, w), jnp.float32)
    for i, ref in enumerate((t_v, s_v, uv_v)):
        for k in range(nk):
            j = i * nk + k
            packed = jnp.where(pair == j, pltpu.roll(ref[pl.ds(k * h, h), :], 2 * j + 1, 1), packed)
    depth_at = 6 * nk
    packed = jnp.where(pair == 3 * nk, pltpu.roll(depth, depth_at + 1, 1), packed)
    pack_v[...] = packed
    half = h // 2
    even_half = lane[:half] % 2 == 0
    last_v[...] = jnp.where(even_half, packed[:half], pltpu.roll(packed[half:], 1, 1))
    first_v[...] = jnp.where(even_half, pltpu.roll(packed[half:], w - 1, 1), packed[:half])

    to_east = pltpu.make_async_remote_copy(
        src_ref=last_v, dst_ref=west_v, send_sem=pack_send.at[0], recv_sem=pack_recv.at[0],
        device_id={"gx": lax.rem(mx + 1, nx)}, device_id_type=MESH,
    )
    to_west = pltpu.make_async_remote_copy(
        src_ref=first_v, dst_ref=east_v, send_sem=pack_send.at[1], recv_sem=pack_recv.at[1],
        device_id={"gx": lax.rem(mx + nx - 1, nx)}, device_id_type=MESH,
    )
    to_east.start()
    to_west.start()

    def rows(ref, row, base=0):
        return ref[pl.ds(base + row, nk, stride=h), :]

    up_v[pl.ds(0, nk), :] = rows(t_v, h - 1)
    up_v[pl.ds(nk, nk), :] = rows(s_v, h - 1)
    up_v[pl.ds(2 * nk, nk), :] = rows(uv_v, h - 1, nk * h)
    up_v[pl.ds(3 * nk, 8), :] = jnp.broadcast_to(depth[h - 1 : h, :], (8, w))
    down_v[pl.ds(0, nk), :] = rows(t_v, 0)
    down_v[pl.ds(nk, nk), :] = rows(s_v, 0)
    down_v[pl.ds(2 * nk, 8), :] = jnp.broadcast_to(depth[0:1, :], (8, w))

    @pl.when(is_top)
    def _():
        up = up_v[...]
        flip = (w - 1) - lax.broadcasted_iota(jnp.int32, up.shape, 1)
        fold_v[mx] = jnp.take_along_axis(up, flip, axis=1)

    to_north = pltpu.make_async_remote_copy(
        src_ref=up_v, dst_ref=south_v, send_sem=row_send.at[0], recv_sem=row_recv.at[0],
        device_id={"gy": lax.rem(my + 1, ny)}, device_id_type=MESH,
    )
    to_south = pltpu.make_async_remote_copy(
        src_ref=down_v, dst_ref=north_v, send_sem=row_send.at[1], recv_sem=row_recv.at[1],
        device_id={"gy": lax.rem(my + ny - 1, ny)}, device_id_type=MESH,
    )

    def fold_copy(d):
        return pltpu.make_async_remote_copy(
            src_ref=fold_v.at[mx], dst_ref=fold_v.at[mx],
            send_sem=fold_send.at[d], recv_sem=fold_recv.at[d],
            device_id={"gx": lax.rem(mx + d + 1, nx)}, device_id_type=MESH,
        )


    @pl.when(jnp.logical_not(is_top))
    def _():
        to_north.start()

    @pl.when(my > 0)
    def _():
        to_south.start()

    @pl.when(is_top)
    def _():
        repeat(nx - 1, lambda d: fold_copy(d).start())

    row = lax.broadcasted_iota(jnp.int32, (h, w), 0)
    depth_east = jnp.where(lane == w - 1, 0.0, jnp.minimum(depth, pltpu.roll(depth, w - 1, 1)))
    depth_north = jnp.where(row == h - 1, 0.0, jnp.minimum(depth, pltpu.roll(depth, h - 1, 0)))

    def level(k, above):
        kf = k.astype(jnp.float32)
        at = pl.ds(pl.multiple_of(k * h, h), h)
        below = pl.ds(pl.multiple_of(jnp.minimum(k + 1, nk - 1) * h, h), h)
        east_near, east_far = face_weights(uv_v[at, :], depth_east > kf)
        north_near, north_far = face_weights(
            uv_v[pl.ds(pl.multiple_of((k + nk) * h, h), h), :], depth_north > kf
        )
        mix = jnp.where(depth_v[...] > kf + 1.0, time_step * vertical_mixing, 0.0)
        gain = g_v[...]
        falls = []
        for ref, out, came in ((t_v, t_out, above[0]), (s_v, s_out, above[1])):
            c = ref[at, :]
            east = east_near * c + east_far * pltpu.roll(c, w - 1, 1)
            north = north_near * c + north_far * pltpu.roll(c, h - 1, 0)
            flow = (pltpu.roll(east, 1, 1) - east) + (pltpu.roll(north, 1, 0) - north)
            fall = mix * (c - ref[below, :])
            out[at, :] = c + (gain * flow + (came - fall))
            falls.append(fall)
        return tuple(falls)

    zero = jnp.zeros((h, w), jnp.float32)
    lax.fori_loop(0, nk, level, (zero, zero))

    to_east.wait()
    to_west.wait()
    mine, east_half, west_half = pack_v[...], east_v[...], west_v[...]
    east_side = jnp.concatenate([east_half, pltpu.roll(east_half, 1, 1)], axis=0)
    west_side = jnp.concatenate([west_half, pltpu.roll(west_half, w - 1, 1)], axis=0)
    even = lane % 2 == 0

    def speeds(cells):
        return jnp.where(
            pair < nk, pltpu.roll(cells, w - 4 * nk, 1), pltpu.roll(cells, w - 2 * nk, 1)
        )

    def column(cells, at):
        return jnp.broadcast_to(cells[:, at : at + 1], (h, w))

    near = jnp.where(even, mine, pltpu.roll(west_side, 1, 1))
    far = jnp.where(even, pltpu.roll(east_side, w - 1, 1), mine)
    speed = jnp.where(even, speeds(mine), pltpu.roll(speeds(west_side), 1, 1))
    shallow = jnp.where(
        even,
        jnp.minimum(column(mine, depth_at), column(east_side, depth_at + 1)),
        jnp.minimum(column(mine, depth_at + 1), column(west_side, depth_at)),
    )
    near_weight, far_weight = face_weights(speed, shallow > (pair % nk).astype(jnp.float32))
    gain = g_v[...]
    edge_gain = jnp.where(even, -column(gain, w - 1), column(gain, 0))
    edge = edge_gain * (near_weight * near + far_weight * far)
    at_edge = (lane == 0) | (lane == w - 1)
    for i, out in enumerate((t_out, s_out)):
        for k in range(nk):
            shift = (w - (2 * (i * nk + k) + 1)) % w
            out[pl.ds(k * h, h), :] += jnp.where(at_edge, pltpu.roll(edge, shift, 1), 0.0)

    level_row = lax.broadcasted_iota(jnp.int32, (nk, w), 0).astype(jnp.float32)

    def north_edge(far_t, far_s, speed, far_depth):
        near_weight, far_weight = face_weights(
            speed, jnp.minimum(up_v[3 * nk : 3 * nk + 1, :], far_depth) > level_row
        )
        for near, far, out in (
            (up_v[pl.ds(0, nk), :], far_t, t_out),
            (up_v[pl.ds(nk, nk), :], far_s, s_out),
        ):
            at = pl.ds(h - 1, nk, stride=h)
            out[at, :] -= g_v[h - 1 : h, :] * (near_weight * near + far_weight * far)

    @pl.when(is_top)
    def _():
        repeat(nx - 1, lambda d: fold_copy(d).wait())
        partner = fold_v[seam_smem[0] // w]
        north_edge(
            partner[:nk],
            partner[nk : 2 * nk],
            0.5 * (up_v[pl.ds(2 * nk, nk), :] - partner[2 * nk : 3 * nk]),
            partner[3 * nk : 3 * nk + 1],
        )

    @pl.when(jnp.logical_not(is_top))
    def _():
        to_north.wait_send()
        to_south.wait_recv()
        north_edge(
            north_v[pl.ds(0, nk), :],
            north_v[pl.ds(nk, nk), :],
            up_v[pl.ds(2 * nk, nk), :],
            north_v[2 * nk : 2 * nk + 1, :],
        )

    @pl.when(my > 0)
    def _():
        to_south.wait_send()
        to_north.wait_recv()
        near_weight, far_weight = face_weights(
            south_v[pl.ds(2 * nk, nk), :],
            jnp.minimum(down_v[2 * nk : 2 * nk + 1, :], south_v[3 * nk : 3 * nk + 1, :]) > level_row,
        )
        for i, out in enumerate((t_out, s_out)):
            at = pl.ds(0, nk, stride=h)
            out[at, :] += g_v[0:1, :] * (
                near_weight * south_v[pl.ds(i * nk, nk), :]
                + far_weight * down_v[pl.ds(i * nk, nk), :]
            )

    repeat(peers, lambda r: part_copy(r).wait())
    totals = part_v[...] + jnp.sum(parts_v[...], axis=0)
    totals = jnp.sum(totals, axis=1, keepdims=True)
    total_area, total_fresh = totals[0:1], totals[1:2]
    salt_fresh, salt_only = totals[2:3], totals[3:4]
    mean_fresh = total_fresh / total_area
    lift = (salt_fresh - mean_fresh * salt_only) / total_area
    virtual = lift - s0_v[...] * (rain_v[...] - mean_fresh)
    s_out[pl.ds(0, h), :] += jnp.where(depth_v[...] > 0.0, time_step / top_thickness * virtual, 0.0)


store_cuts = 4


def store_kernel(t_ref, s_ref, t_out, s_out, sems):
    step = t_ref.shape[0] // store_cuts
    copies = [
        pltpu.make_async_copy(
            src.at[pl.ds(i * step, step)], dst.at[pl.ds(i * step, step)], sems.at[2 * i + n]
        )
        for i in range(store_cuts)
        for n, (src, dst) in enumerate(((t_ref, t_out), (s_ref, s_out)))
    ]
    for copy in copies:
        copy.start()
    for copy in copies:
        copy.wait()


def shards(nx, ny, t, s, uv, sea, layers, area, rain, seam):
    nk, h, w = t.shape
    assert w == 128 and h % 16 == 0 and nk % 8 == 0 and 6 * nk + 2 <= w
    f32 = jnp.float32
    peers = nx * ny - 1
    half_plane = pltpu.VMEM((h // 2, w), f32)
    any_space = pl.BlockSpec(memory_space=pl.ANY)
    dma = pltpu.SemaphoreType.DMA
    plane = pltpu.VMEM((h, w), f32)
    t_next, s_next = pl.pallas_call(
        functools.partial(kernel, nx, ny, nk, h, w),
        out_shape=[pltpu.VMEM((nk * h, w), f32)] * 2,
        in_specs=[any_space] * 7 + [pl.BlockSpec(memory_space=pltpu.SMEM)],
        out_specs=[pl.BlockSpec(memory_space=pltpu.VMEM)] * 2,
        scratch_shapes=[
            pltpu.VMEM((nk * h, w), f32),
            pltpu.VMEM((nk * h, w), f32),
            pltpu.VMEM((2 * nk * h, w), f32),
            pltpu.VMEM((h, w), jnp.int32),
            pltpu.VMEM((h, w), jnp.int32),
            plane, plane, plane, plane, plane,
            plane, half_plane, half_plane, half_plane, half_plane,
            pltpu.VMEM((3 * nk + 8, w), f32),
            pltpu.VMEM((2 * nk + 8, w), f32),
            pltpu.VMEM((3 * nk + 8, w), f32),
            pltpu.VMEM((2 * nk + 8, w), f32),
            pltpu.VMEM((nx, 3 * nk + 8, w), f32),
            pltpu.VMEM((8, w), f32),
            pltpu.VMEM((peers, 8, w), f32),
            dma((9,)), dma((2,)), dma((2,)), dma((2,)), dma((2,)),
            dma((nx - 1,)), dma((nx - 1,)), dma((peers,)), dma((peers,)),
        ],
        compiler_params=pltpu.CompilerParams(
            collective_id=0, has_side_effects=True, vmem_limit_bytes=65990000
        ),
        name="tracer_step",
    )(
        t.reshape(nk * h, w), s.reshape(nk * h, w), uv.reshape(2 * nk * h, w),
        sea, layers, area, rain, seam,
    )
    t_next, s_next = pl.pallas_call(
        store_kernel,
        out_shape=[jax.ShapeDtypeStruct((nk * h, w), f32)] * 2,
        in_specs=[any_space] * 2,
        out_specs=[any_space] * 2,
        scratch_shapes=[dma((2 * store_cuts,))],
        compiler_params=pltpu.CompilerParams(vmem_limit_bytes=8 << 20),
        name="store",
    )(t_next, s_next)
    return t_next.reshape(t.shape), s_next.reshape(s.shape)


def solution(mesh):
    in_specs = (
        P("groups", "gy", "gx"),
        P("groups", "gy", "gx"),
        P("groups", None, "gy", "gx"),
        P("gy", "gx"),
        P("gy", "gx"),
        P("gy", "gx"),
        P("gy", "gx"),
        P("gx"),
    )
    out_specs = (P("groups", "gy", "gx"), P("groups", "gy", "gx"))
    return jax.shard_map(
        functools.partial(shards, mesh.shape["gx"], mesh.shape["gy"]),
        mesh=mesh, in_specs=in_specs, out_specs=out_specs, check_vma=False,
    )
```

```python
import functools

import jax
import jax.numpy as jnp
from jax import lax
from jax.experimental import pallas as pl
from jax.experimental.pallas import tpu as pltpu
from jax.sharding import PartitionSpec as P

time_step = 0.25
diffusivity = 0.5
vertical_mixing = 0.3
top_thickness = 0.5

MESH = pl.DeviceIdType.MESH


def repeat(count, body):
    if count <= 16:
        for i in range(count):
            body(i)
    else:
        pl.loop(0, count)(body)


def face_weights(speed, open_face):
    near_weight = jnp.where(open_face, jnp.maximum(speed, 0.0) + diffusivity, 0.0)
    far_weight = jnp.where(open_face, jnp.minimum(speed, 0.0) - diffusivity, 0.0)
    return near_weight, far_weight


def kernel(
    nx, ny, nk, h, w,
    t_hbm, s_hbm, uv_hbm, sea_hbm, lay_hbm, area_hbm, rain_hbm, seam_smem,
    t_out, s_out,
    t_v, s_v, uv_v, sea_v, lay_v, area_v, rain_v, s0_v, g_v, depth_v,
    pack_v, last_v, first_v, east_v, west_v, up_v, down_v, south_v, north_v, fold_v,
    part_v, parts_v,
    load_sems, pack_send, pack_recv, row_send, row_recv, fold_send, fold_recv,
    part_send, part_recv,
):
    mx, my = lax.axis_index("gx"), lax.axis_index("gy")
    is_top = my == ny - 1
    peers = nx * ny - 1

    def peer(r):
        r = r + 1
        return {"gx": lax.rem(mx + r // ny, nx), "gy": lax.rem(my + r % ny, ny)}

    barrier = pltpu.get_barrier_semaphore()

    def greet(r):
        pl.semaphore_signal(barrier, inc=1, device_id=peer(r), device_id_type=MESH)

    repeat(peers, greet)

    loads = [
        pltpu.make_async_copy(src, dst, load_sems.at[i])
        for i, (src, dst) in enumerate(
            [
                (area_hbm, area_v),
                (sea_hbm, sea_v),
                (rain_hbm, rain_v),
                (s_hbm.at[pl.ds(0, h)], s0_v),
                (lay_hbm, lay_v),
                (t_hbm, t_v),
                (s_hbm, s_v),
                (uv_hbm.at[pl.ds(0, nk * h)], uv_v.at[pl.ds(0, nk * h)]),
                (uv_hbm.at[pl.ds(nk * h, nk * h)], uv_v.at[pl.ds(nk * h, nk * h)]),
            ]
        )
    ]
    for load in loads:
        load.start()

    for load in loads[:4]:
        load.wait()
    area = area_v[...]
    sea = sea_v[...]
    wet_area = area * sea.astype(jnp.float32)
    surface = s0_v[...]
    fresh = wet_area * rain_v[...]
    row8 = lax.broadcasted_iota(jnp.int32, (8, w), 0)
    part = jnp.zeros((8, w), jnp.float32)
    for i, term in enumerate((wet_area, fresh, fresh * surface, wet_area * surface)):
        part = jnp.where(row8 == i, jnp.sum(term, axis=0, keepdims=True), part)
    part_v[...] = part
    gain = time_step / area
    g_v[...] = gain

    pl.semaphore_wait(barrier, peers)

    def part_copy(r):
        return pltpu.make_async_remote_copy(
            src_ref=part_v, dst_ref=parts_v.at[r],
            send_sem=part_send.at[r], recv_sem=part_recv.at[r],
            device_id=peer(r), device_id_type=MESH,
        )

    repeat(peers, lambda r: part_copy(r).start())

    for load in loads[4:]:
        load.wait()
    depth = (sea * lay_v[...]).astype(jnp.float32)
    depth_v[...] = depth

    lane = lax.broadcasted_iota(jnp.int32, (h, w), 1)
    pair = lane // 2
    packed = jnp.zeros((h, w), jnp.float32)
    for i, ref in enumerate((t_v, s_v, uv_v)):
        for k in range(nk):
            j = i * nk + k
            packed = jnp.where(pair == j, pltpu.roll(ref[pl.ds(k * h, h), :], 2 * j + 1, 1), packed)
    depth_at = 6 * nk
    packed = jnp.where(pair == 3 * nk, pltpu.roll(depth, depth_at + 1, 1), packed)
    pack_v[...] = packed
    half = h // 2
    even_half = lane[:half] % 2 == 0
    last_v[...] = jnp.where(even_half, packed[:half], pltpu.roll(packed[half:], 1, 1))
    first_v[...] = jnp.where(even_half, pltpu.roll(packed[half:], w - 1, 1), packed[:half])

    to_east = pltpu.make_async_remote_copy(
        src_ref=last_v, dst_ref=west_v, send_sem=pack_send.at[0], recv_sem=pack_recv.at[0],
        device_id={"gx": lax.rem(mx + 1, nx)}, device_id_type=MESH,
    )
    to_west = pltpu.make_async_remote_copy(
        src_ref=first_v, dst_ref=east_v, send_sem=pack_send.at[1], recv_sem=pack_recv.at[1],
        device_id={"gx": lax.rem(mx + nx - 1, nx)}, device_id_type=MESH,
    )
    to_east.start()
    to_west.start()

    def rows(ref, row, base=0):
        return ref[pl.ds(base + row, nk, stride=h), :]

    up_v[pl.ds(0, nk), :] = rows(t_v, h - 1)
    up_v[pl.ds(nk, nk), :] = rows(s_v, h - 1)
    up_v[pl.ds(2 * nk, nk), :] = rows(uv_v, h - 1, nk * h)
    up_v[pl.ds(3 * nk, 8), :] = jnp.broadcast_to(depth[h - 1 : h, :], (8, w))
    down_v[pl.ds(0, nk), :] = rows(t_v, 0)
    down_v[pl.ds(nk, nk), :] = rows(s_v, 0)
    down_v[pl.ds(2 * nk, 8), :] = jnp.broadcast_to(depth[0:1, :], (8, w))

    @pl.when(is_top)
    def _():
        up = up_v[...]
        flip = (w - 1) - lax.broadcasted_iota(jnp.int32, up.shape, 1)
        fold_v[mx] = jnp.take_along_axis(up, flip, axis=1)

    to_north = pltpu.make_async_remote_copy(
        src_ref=up_v, dst_ref=south_v, send_sem=row_send.at[0], recv_sem=row_recv.at[0],
        device_id={"gy": lax.rem(my + 1, ny)}, device_id_type=MESH,
    )
    to_south = pltpu.make_async_remote_copy(
        src_ref=down_v, dst_ref=north_v, send_sem=row_send.at[1], recv_sem=row_recv.at[1],
        device_id={"gy": lax.rem(my + ny - 1, ny)}, device_id_type=MESH,
    )

    def fold_copy(d):
        return pltpu.make_async_remote_copy(
            src_ref=fold_v.at[mx], dst_ref=fold_v.at[mx],
            send_sem=fold_send.at[d], recv_sem=fold_recv.at[d],
            device_id={"gx": lax.rem(mx + d + 1, nx)}, device_id_type=MESH,
        )


    @pl.when(jnp.logical_not(is_top))
    def _():
        to_north.start()

    @pl.when(my > 0)
    def _():
        to_south.start()

    @pl.when(is_top)
    def _():
        repeat(nx - 1, lambda d: fold_copy(d).start())

    row = lax.broadcasted_iota(jnp.int32, (h, w), 0)
    depth_east = jnp.where(lane == w - 1, 0.0, jnp.minimum(depth, pltpu.roll(depth, w - 1, 1)))
    depth_north = jnp.where(row == h - 1, 0.0, jnp.minimum(depth, pltpu.roll(depth, h - 1, 0)))

    def level(k, above):
        kf = k.astype(jnp.float32)
        at = pl.ds(pl.multiple_of(k * h, h), h)
        below = pl.ds(pl.multiple_of(jnp.minimum(k + 1, nk - 1) * h, h), h)
        east_near, east_far = face_weights(uv_v[at, :], depth_east > kf)
        north_near, north_far = face_weights(
            uv_v[pl.ds(pl.multiple_of((k + nk) * h, h), h), :], depth_north > kf
        )
        mix = jnp.where(depth_v[...] > kf + 1.0, time_step * vertical_mixing, 0.0)
        gain = g_v[...]
        falls = []
        for ref, out, came in ((t_v, t_out, above[0]), (s_v, s_out, above[1])):
            c = ref[at, :]
            east = east_near * c + east_far * pltpu.roll(c, w - 1, 1)
            north = north_near * c + north_far * pltpu.roll(c, h - 1, 0)
            flow = (pltpu.roll(east, 1, 1) - east) + (pltpu.roll(north, 1, 0) - north)
            fall = mix * (c - ref[below, :])
            out[at, :] = c + (gain * flow + (came - fall))
            falls.append(fall)
        return tuple(falls)

    zero = jnp.zeros((h, w), jnp.float32)
    lax.fori_loop(0, nk, level, (zero, zero))

    level_row = lax.broadcasted_iota(jnp.int32, (nk, w), 0).astype(jnp.float32)

    def north_edge(far_t, far_s, speed, far_depth):
        near_weight, far_weight = face_weights(
            speed, jnp.minimum(up_v[3 * nk : 3 * nk + 1, :], far_depth) > level_row
        )
        for near, far, out in (
            (up_v[pl.ds(0, nk), :], far_t, t_out),
            (up_v[pl.ds(nk, nk), :], far_s, s_out),
        ):
            at = pl.ds(h - 1, nk, stride=h)
            out[at, :] -= g_v[h - 1 : h, :] * (near_weight * near + far_weight * far)

    @pl.when(jnp.logical_not(is_top))
    def _():
        to_north.wait_send()
        to_south.wait_recv()
        north_edge(
            north_v[pl.ds(0, nk), :],
            north_v[pl.ds(nk, nk), :],
            up_v[pl.ds(2 * nk, nk), :],
            north_v[2 * nk : 2 * nk + 1, :],
        )

    @pl.when(my > 0)
    def _():
        to_south.wait_send()
        to_north.wait_recv()
        near_weight, far_weight = face_weights(
            south_v[pl.ds(2 * nk, nk), :],
            jnp.minimum(down_v[2 * nk : 2 * nk + 1, :], south_v[3 * nk : 3 * nk + 1, :]) > level_row,
        )
        for i, out in enumerate((t_out, s_out)):
            at = pl.ds(0, nk, stride=h)
            out[at, :] += g_v[0:1, :] * (
                near_weight * south_v[pl.ds(i * nk, nk), :]
                + far_weight * down_v[pl.ds(i * nk, nk), :]
            )

    to_east.wait()
    to_west.wait()
    mine, east_half, west_half = pack_v[...], east_v[...], west_v[...]
    east_side = jnp.concatenate([east_half, pltpu.roll(east_half, 1, 1)], axis=0)
    west_side = jnp.concatenate([west_half, pltpu.roll(west_half, w - 1, 1)], axis=0)
    even = lane % 2 == 0

    def speeds(cells):
        return jnp.where(
            pair < nk, pltpu.roll(cells, w - 4 * nk, 1), pltpu.roll(cells, w - 2 * nk, 1)
        )

    def column(cells, at):
        return jnp.broadcast_to(cells[:, at : at + 1], (h, w))

    near = jnp.where(even, mine, pltpu.roll(west_side, 1, 1))
    far = jnp.where(even, pltpu.roll(east_side, w - 1, 1), mine)
    speed = jnp.where(even, speeds(mine), pltpu.roll(speeds(west_side), 1, 1))
    shallow = jnp.where(
        even,
        jnp.minimum(column(mine, depth_at), column(east_side, depth_at + 1)),
        jnp.minimum(column(mine, depth_at + 1), column(west_side, depth_at)),
    )
    near_weight, far_weight = face_weights(speed, shallow > (pair % nk).astype(jnp.float32))
    gain = g_v[...]
    edge_gain = jnp.where(even, -column(gain, w - 1), column(gain, 0))
    edge = edge_gain * (near_weight * near + far_weight * far)
    at_edge = (lane == 0) | (lane == w - 1)
    for i, out in enumerate((t_out, s_out)):
        for k in range(nk):
            shift = (w - (2 * (i * nk + k) + 1)) % w
            out[pl.ds(k * h, h), :] += jnp.where(at_edge, pltpu.roll(edge, shift, 1), 0.0)

    @pl.when(is_top)
    def _():
        repeat(nx - 1, lambda d: fold_copy(d).wait())
        partner = fold_v[seam_smem[0] // w]
        north_edge(
            partner[:nk],
            partner[nk : 2 * nk],
            0.5 * (up_v[pl.ds(2 * nk, nk), :] - partner[2 * nk : 3 * nk]),
            partner[3 * nk : 3 * nk + 1],
        )

    repeat(peers, lambda r: part_copy(r).wait())
    totals = part_v[...] + jnp.sum(parts_v[...], axis=0)
    totals = jnp.sum(totals, axis=1, keepdims=True)
    total_area, total_fresh = totals[0:1], totals[1:2]
    salt_fresh, salt_only = totals[2:3], totals[3:4]
    mean_fresh = total_fresh / total_area
    lift = (salt_fresh - mean_fresh * salt_only) / total_area
    virtual = lift - s0_v[...] * (rain_v[...] - mean_fresh)
    s_out[pl.ds(0, h), :] += jnp.where(depth_v[...] > 0.0, time_step / top_thickness * virtual, 0.0)


store_cuts = 1


def store_kernel(t_ref, s_ref, t_out, s_out, sems):
    step = t_ref.shape[0] // store_cuts
    copies = [
        pltpu.make_async_copy(
            src.at[pl.ds(i * step, step)], dst.at[pl.ds(i * step, step)], sems.at[2 * i + n]
        )
        for i in range(store_cuts)
        for n, (src, dst) in enumerate(((t_ref, t_out), (s_ref, s_out)))
    ]
    for copy in copies:
        copy.start()
    for copy in copies:
        copy.wait()


def shards(nx, ny, t, s, uv, sea, layers, area, rain, seam):
    nk, h, w = t.shape
    assert w == 128 and h % 16 == 0 and nk % 8 == 0 and 6 * nk + 2 <= w
    f32 = jnp.float32
    peers = nx * ny - 1
    half_plane = pltpu.VMEM((h // 2, w), f32)
    any_space = pl.BlockSpec(memory_space=pl.ANY)
    dma = pltpu.SemaphoreType.DMA
    plane = pltpu.VMEM((h, w), f32)
    t_next, s_next = pl.pallas_call(
        functools.partial(kernel, nx, ny, nk, h, w),
        out_shape=[pltpu.VMEM((nk * h, w), f32)] * 2,
        in_specs=[any_space] * 7 + [pl.BlockSpec(memory_space=pltpu.SMEM)],
        out_specs=[pl.BlockSpec(memory_space=pltpu.VMEM)] * 2,
        scratch_shapes=[
            pltpu.VMEM((nk * h, w), f32),
            pltpu.VMEM((nk * h, w), f32),
            pltpu.VMEM((2 * nk * h, w), f32),
            pltpu.VMEM((h, w), jnp.int32),
            pltpu.VMEM((h, w), jnp.int32),
            plane, plane, plane, plane, plane,
            plane, half_plane, half_plane, half_plane, half_plane,
            pltpu.VMEM((3 * nk + 8, w), f32),
            pltpu.VMEM((2 * nk + 8, w), f32),
            pltpu.VMEM((3 * nk + 8, w), f32),
            pltpu.VMEM((2 * nk + 8, w), f32),
            pltpu.VMEM((nx, 3 * nk + 8, w), f32),
            pltpu.VMEM((8, w), f32),
            pltpu.VMEM((peers, 8, w), f32),
            dma((9,)), dma((2,)), dma((2,)), dma((2,)), dma((2,)),
            dma((nx - 1,)), dma((nx - 1,)), dma((peers,)), dma((peers,)),
        ],
        compiler_params=pltpu.CompilerParams(
            collective_id=0, has_side_effects=True, vmem_limit_bytes=65990000
        ),
        name="tracer_step",
    )(
        t.reshape(nk * h, w), s.reshape(nk * h, w), uv.reshape(2 * nk * h, w),
        sea, layers, area, rain, seam,
    )
    t_next, s_next = pl.pallas_call(
        store_kernel,
        out_shape=[jax.ShapeDtypeStruct((nk * h, w), f32)] * 2,
        in_specs=[any_space] * 2,
        out_specs=[any_space] * 2,
        scratch_shapes=[dma((2 * store_cuts,))],
        compiler_params=pltpu.CompilerParams(vmem_limit_bytes=8 << 20),
        name="store",
    )(t_next, s_next)
    return t_next.reshape(t.shape), s_next.reshape(s.shape)


def solution(mesh):
    in_specs = (
        P("groups", "gy", "gx"),
        P("groups", "gy", "gx"),
        P("groups", None, "gy", "gx"),
        P("gy", "gx"),
        P("gy", "gx"),
        P("gy", "gx"),
        P("gy", "gx"),
        P("gx"),
    )
    out_specs = (P("groups", "gy", "gx"), P("groups", "gy", "gx"))
    return jax.shard_map(
        functools.partial(shards, mesh.shape["gx"], mesh.shape["gy"]),
        mesh=mesh, in_specs=in_specs, out_specs=out_specs, check_vma=False,
    )
```
